32 devices in a mesh: dp: 1 (over z), col: 4 (over y), row: 8 (over x, core).
Axes of the slice: x: 4, y: 4, z: 1, core: 2. Of those that a mesh axis runs over, the one named last changes fastest.
The devices are a block of a 4x4x8 slice.
Arguments:
- pair_rep: bfloat16 [1536, 1536, 64], P(('dp', 'row'), 'col')
- pair_mask: int32 [1536, 1536], P(('dp', 'row'), 'col')
- norm_in: bfloat16 [64], replicated
- proj_left: bfloat16 [64, 64], replicated
- gate_left: bfloat16 [64, 64], replicated
- proj_right: bfloat16 [64, 64], replicated
- gate_right: bfloat16 [64, 64], replicated
- proj_gate: bfloat16 [64, 64], replicated
- norm_out: bfloat16 [64], replicated
- proj_out: bfloat16 [64, 64], replicated
Outputs:
- output: bfloat16 [1536, 1536, 64], P(('dp', 'row'), 'col')
All inputs are finite; a program needn't handle non-finite values.
Results may differ from the reference program's by a relative error of at most 0.00624021.
Values are sent between devices in bfloat16 or wider.
A program may use at most 768 MiB of HBM per device.

```python
import jax
import jax.numpy as jnp
from jax import lax

SEQ = 1536
CZ = 64
CHAN = 64
ROW_BLOCK = SEQ // 8
LN_EPS = 1e-5


def layer_norm(values, gain_vec, red_axis):
    centre = values - jnp.mean(values, axis=red_axis, keepdims=True)
    spread = jnp.mean(centre * centre, axis=red_axis, keepdims=True)
    return centre * lax.rsqrt(spread + LN_EPS) * gain_vec


def normal_weight(rng_key, w_shape, std_scale):
    return (jax.random.normal(rng_key, w_shape, jnp.float32) * std_scale).astype(jnp.bfloat16)


def gain_vector(rng_key, gain_width):
    return (1.0 + 0.3 * jax.random.normal(rng_key, (gain_width,), jnp.float32)).astype(jnp.bfloat16)


def setup_inputs(seed: int = 0, part: int = 0) -> dict:
    part_key = jax.random.fold_in(jax.random.key(seed), part)
    pair_key, mask_key = jax.random.split(part_key)
    weight_keys = jax.random.split(jax.random.key(seed + 1), 8)
    pair_rep = jax.random.normal(pair_key, (SEQ, SEQ, CZ), jnp.float32).astype(jnp.bfloat16)
    residue_ok = (jax.random.randint(mask_key, (SEQ,), 0, 10) != 0).astype(jnp.int32)
    pair_mask = residue_ok[:, None] * residue_ok[None, :]
    return dict(
        pair_rep=pair_rep,
        pair_mask=pair_mask,
        norm_in=gain_vector(weight_keys[0], CZ),
        proj_left=normal_weight(weight_keys[1], (CZ, CHAN), CZ ** -0.5),
        gate_left=normal_weight(weight_keys[2], (CZ, CHAN), CZ ** -0.5),
        proj_right=normal_weight(weight_keys[3], (CZ, CHAN), CZ ** -0.5),
        gate_right=normal_weight(weight_keys[4], (CZ, CHAN), CZ ** -0.5),
        proj_gate=normal_weight(weight_keys[5], (CZ, CZ), CZ ** -0.5),
        norm_out=gain_vector(weight_keys[6], CHAN),
        proj_out=normal_weight(weight_keys[7], (CHAN, CZ), 2.0 * CHAN ** -0.5),
    )


def reference(pair_rep, pair_mask, norm_in, proj_left, gate_left, proj_right, gate_right, proj_gate, norm_out, proj_out):
    pair_f = pair_rep.astype(jnp.float32)
    normed = layer_norm(pair_f, norm_in.astype(jnp.float32), -1).astype(jnp.bfloat16)
    flat_x = normed.reshape(SEQ * SEQ, CZ)
    keep_f = pair_mask.astype(jnp.float32).reshape(SEQ * SEQ, 1)

    def gated_proj(w_value, w_gate):
        value_f = jnp.dot(flat_x, w_value, preferred_element_type=jnp.float32)
        gate_vals = jax.nn.sigmoid(jnp.dot(flat_x, w_gate, preferred_element_type=jnp.float32))
        return (keep_f * gate_vals * value_f).astype(jnp.bfloat16).T.reshape(CHAN, SEQ, SEQ)

    left_op = gated_proj(proj_left, gate_left)
    right_op = gated_proj(proj_right, gate_right)
    out_gate = jax.nn.sigmoid(jnp.dot(flat_x, proj_gate, preferred_element_type=jnp.float32))
    gate_blocks = out_gate.reshape(8, ROW_BLOCK, SEQ, CZ)
    left_blocks = left_op.reshape(CHAN, 8, ROW_BLOCK, SEQ).transpose(1, 0, 2, 3)
    pair_blocks = pair_f.reshape(8, ROW_BLOCK, SEQ, CZ)
    gain_out = norm_out.astype(jnp.float32)[:, None, None]

    def channel_product(operands):
        return jnp.dot(operands[0], operands[1].T, preferred_element_type=jnp.float32)

    def row_block(operands):
        left_blk, gate_blk, pair_blk = operands
        contracted = lax.map(channel_product, (left_blk, right_op))
        normed_o = layer_norm(contracted, gain_out, 0).astype(jnp.bfloat16)
        update = jnp.dot(normed_o.reshape(CHAN, ROW_BLOCK * SEQ).T, proj_out, preferred_element_type=jnp.float32)
        return (pair_blk + gate_blk * update.reshape(ROW_BLOCK, SEQ, CZ)).astype(jnp.bfloat16)

    new_pair = lax.map(row_block, (left_blocks, gate_blocks, pair_blocks))
    return new_pair.reshape(SEQ, SEQ, CZ)
```

```python
import functools

import jax
import jax.numpy as jnp
from jax import lax
from jax.experimental import pallas as pl
from jax.experimental.pallas import tpu as pltpu
from jax.sharding import PartitionSpec as P

LN_EPS = 1e-5
F32 = jnp.float32
BF16 = jnp.bfloat16
MESH = pl.DeviceIdType.MESH
VMEM_LIMIT = 60 * 1024 * 1024
PER_HALF = 1
FRONT_ROWS = 16


def normalize(values, gain):
    centre = values - jnp.mean(values, axis=0, keepdims=True)
    spread = jnp.mean(centre * centre, axis=0, keepdims=True)
    return (centre * lax.rsqrt(spread + LN_EPS) * gain).astype(BF16)


def front_kernel(z_ref, m_ref, g_ref, w_ref, a_ref, b_ref, sa, sb):
    rows, chan, cols = z_ref.shape
    tiles = sa.shape[0]
    pitch = sa.shape[1] // rows
    hid = w_ref.shape[0] // 4

    def one_row(i, _):
        xn = normalize(z_ref[i].astype(F32), g_ref[...])
        p = jnp.dot(w_ref[...], xn, preferred_element_type=F32)
        keep = m_ref[pl.ds(i, 1), :].astype(F32)
        left = keep * jax.nn.sigmoid(p[hid:2 * hid]) * p[:hid]
        right = keep * jax.nn.sigmoid(p[3 * hid:]) * p[2 * hid:3 * hid]
        at = pl.ds(pl.multiple_of(i * pitch, 8), hid)
        for t in range(tiles):
            sa[t, at, :] = left[:, t * 128:(t + 1) * 128]
            sb[t, at, :] = right[:, t * 128:(t + 1) * 128]
        return 0

    lax.fori_loop(0, rows, one_row, 0, unroll=2)

    def one_channel(c, _):
        for t in range(tiles):
            at = slice(t * 128, (t + 1) * 128)
            a_ref[c, :, at] = sa[t, pl.ds(c, rows, stride=pitch), :].astype(BF16)
            b_ref[c, :, at] = sb[t, pl.ds(c, rows, stride=pitch), :].astype(BF16)
        return 0

    lax.fori_loop(0, hid, one_channel, 0, unroll=4)


def front(z_t, mask, g_in, w_cat):
    rows, chan, cols = z_t.shape
    hid = w_cat.shape[0] // 4
    fr = FRONT_ROWS
    scratch = pltpu.VMEM((cols // 128, fr * (hid + 8), 128), F32)
    out = jax.ShapeDtypeStruct((hid, rows, cols), BF16)
    out_spec = pl.BlockSpec((hid, fr, cols), lambda i: (0, i, 0))
    return pl.pallas_call(
        front_kernel,
        grid=(rows // fr,),
        in_specs=[
            pl.BlockSpec((fr, chan, cols), lambda i: (i, 0, 0)),
            pl.BlockSpec((fr, cols), lambda i: (i, 0)),
            pl.BlockSpec((chan, 1), lambda i: (0, 0)),
            pl.BlockSpec(w_cat.shape, lambda i: (0, 0)),
        ],
        out_specs=[out_spec, out_spec],
        out_shape=[out, out],
        scratch_shapes=[scratch, scratch],
        compiler_params=pltpu.CompilerParams(vmem_limit_bytes=VMEM_LIMIT),
        name="front",
    )(z_t, mask, g_in, w_cat)


def main_kernel(nc, a_own, b_own, z_hbm, g_in, w_gate, g_out, w_out, out_hbm, a_land, b_land,
                a_buf, b_buf, o_buf, z_buf, sem_sp, sem_rp, sem_sa, sem_ra, sem_se, sem_re,
                sem_sd, sem_rd, sem_l, sem_z):
    hid, rows, cols = a_own.shape
    h = PER_HALF
    ch = 2 * h
    n = hid // ch
    half = hid // 2
    relay0 = 8 * hid
    dp, y, r = lax.axis_index("dp"), lax.axis_index("col"), lax.axis_index("row")
    cores = 2
    x, core = r // cores, r % cores
    up = lambda v: (v + 1) % nc
    dn = lambda v: (v + nc - 1) % nc
    xp, xm = (dp, y, up(x) * cores + core), (dp, y, dn(x) * cores + core)
    yp, ym = (dp, up(y), r), (dp, dn(y), r)
    mate = (dp, y, x * cores + 1 - core)
    cls = (y + nc - x) % nc
    is0 = cls == 0
    eq = [(cls == k).astype(jnp.int32) for k in range(4)]
    pick = lambda c0, c1, c2, c3: eq[0] * c0 + eq[1] * c1 + eq[2] * c2 + eq[3] * c3

    barrier = pltpu.get_barrier_semaphore()
    for dev in (xp, xm, yp, ym, mate):
        pl.semaphore_signal(barrier, inc=1, device_id=dev, device_id_type=MESH)
    pl.semaphore_wait(barrier, 5)

    load_z = pltpu.make_async_copy(z_hbm, z_buf, sem_z.at[0])
    load_z.start()

    dirs = [pick(1, 3, 0, 2), pick(0, 1, 1, 0), pick(2, 0, 3, 1), pick(3, 2, 2, 3)]
    hops = [pick(2, 1, 1, 1), pick(2, 1, 1, 1), pick(3, 2, 2, 2), pick(3, 4, 2, 4)]
    src_relay = [3, 2, pick(0, 0, 1, 1), pick(1, 2, 0, 3)]
    tgt = [pick(4, 3, 0, 2), pick(4, 1, 1, 0), pick(2, 0, 5, 1), pick(3, 4, 5, 5)]

    def dev_of(d):
        dx = (d == 0).astype(jnp.int32) + 3 * (d == 1).astype(jnp.int32)
        dy = (d == 2).astype(jnp.int32) + 3 * (d == 3).astype(jnp.int32)
        return (dp, (y + dy) % nc, ((x + dx) % nc) * cores + core)

    perm_devs = [dev_of(d) for d in dirs]

    def tgt_at(k, t):
        to_e = tgt[k] // 4
        return (1 - to_e) * (relay0 + tgt[k] * half + t * h) + to_e * ((2 * t + tgt[k] - 4) * h)

    def remote(src, dst, send, recv, dev):
        return pltpu.make_async_remote_copy(src_ref=src, dst_ref=dst, send_sem=send, recv_sem=recv,
                                            device_id=dev, device_id_type=MESH)

    def perm_copy(k, t, src):
        return remote(src, b_land.at[pl.ds(tgt_at(k, t), h)], sem_sp.at[k, t], sem_rp.at[tgt[k], t], perm_devs[k])

    def got_perm(which, t):
        pltpu.make_async_copy(b_land.at[pl.ds(0, h)], b_land.at[pl.ds(0, h)], sem_rp.at[which, t]).wait()

    def land(buf, slot, t, f=0, count=ch):
        return buf.at[pl.ds(slot * hid + t * ch + f * h, count)]

    def got(buf, sem, count):
        pltpu.make_async_copy(buf.at[pl.ds(0, count)], buf.at[pl.ds(0, count)], sem).wait()

    def own(buf, t, count=ch, f=0):
        return buf.at[pl.ds(t * ch + f * h, count)]

    def a_own_sends(t):
        return [
            remote(own(a_own, t), land(a_land, 0, t), sem_sa.at[0, t], sem_ra.at[0, t], yp),
            remote(own(a_own, t), land(a_land, 1, t), sem_sa.at[1, t], sem_ra.at[1, t], ym),
        ]

    def e_own_sends(t, src):
        return [
            remote(src, land(b_land, 1, t), sem_se.at[0, t], sem_re.at[0, t], xp),
            remote(src, land(b_land, 2, t), sem_se.at[1, t], sem_re.at[1, t], xm),
            remote(src, land(b_land, 4, t), sem_sd.at[0, t], sem_rd.at[0, t], mate),
        ]

    def local_loads(t, slot):
        put_a = lambda rel: a_buf.at[slot, :, :, pl.ds(rel * cols, cols)]
        out = [
            (own(a_own, t), put_a(0)),
            (land(a_land, 0, t), put_a(3)),
            (land(a_land, 1, t), put_a(1)),
            (land(a_land, 2, t), put_a(2)),
        ]
        for k, delta in enumerate((0, 3, 1, 2)):
            rel = (cls + nc - delta) % nc
            where = pl.ds(pl.multiple_of(rel * cols, 128), cols)
            if k > 0:
                out.append((land(b_land, k, t), b_buf.at[slot, :, core, :, where]))
            out.append((land(b_land, 4 + k, t), b_buf.at[slot, :, 1 - core, :, where]))
        return [pltpu.make_async_copy(s, d, sem_l.at[slot, j]) for j, (s, d) in enumerate(out)]

    def own_e_load(t, slot, src):
        where = pl.ds(pl.multiple_of(cls * cols, 128), cols)
        return pltpu.make_async_copy(src, b_buf.at[slot, :, core, :, where], sem_l.at[slot, 11])

    def at_lag(q, lag, fn):
        t = q - lag

        @pl.when(jnp.logical_and(t >= 0, t < n))
        def _():
            fn(t)

    def step(q, _):
        for k in range(4):
            def send(t, k=k):
                if k < 2:
                    @pl.when(is0)
                    def _():
                        got_perm(src_relay[k], t)
                        perm_copy(k, t, b_land.at[pl.ds(relay0 + src_relay[k] * half + t * h, h)]).start()

                    @pl.when(jnp.logical_not(is0))
                    def _():
                        perm_copy(k, t, own(b_own, t, h, k)).start()
                else:
                    got_perm(src_relay[k], t)
                    perm_copy(k, t, b_land.at[pl.ds(relay0 + src_relay[k] * half + t * h, h)]).start()

            at_lag(q, hops[k] - 1, send)

        def e_own(t):
            @pl.when(is0)
            def _():
                for c in e_own_sends(t, own(b_own, t)):
                    c.start()

            @pl.when(jnp.logical_not(is0))
            def _():
                got_perm(4, t)
                got_perm(5, t)
                for c in e_own_sends(t, land(b_land, 0, t)):
                    c.start()

        at_lag(q, 4, e_own)

        def a_first(t):
            for c in a_own_sends(t):
                c.start()

        at_lag(q, 3, a_first)

        def e_fwd(t):
            got(b_land, sem_re.at[0, t], ch)
            remote(land(b_land, 1, t, 0, h), land(b_land, 3, t, 0, h), sem_se.at[2, t], sem_re.at[2, t], xp).start()
            remote(land(b_land, 1, t), land(b_land, 5, t), sem_sd.at[1, t], sem_rd.at[1, t], mate).start()
            got(b_land, sem_re.at[1, t], ch)
            remote(land(b_land, 2, t, 1, h), land(b_land, 3, t, 1, h), sem_se.at[3, t], sem_re.at[3, t], xm).start()
            remote(land(b_land, 2, t), land(b_land, 6, t), sem_sd.at[2, t], sem_rd.at[2, t], mate).start()

        at_lag(q, 5, e_fwd)

        def a_fwd(t):
            got(a_land, sem_ra.at[0, t], ch)
            remote(land(a_land, 0, t, 0, h), land(a_land, 2, t, 0, h), sem_sa.at[2, t], sem_ra.at[2, t], yp).start()
            got(a_land, sem_ra.at[1, t], ch)
            remote(land(a_land, 1, t, 1, h), land(a_land, 2, t, 1, h), sem_sa.at[3, t], sem_ra.at[3, t], ym).start()

        at_lag(q, 4, a_fwd)

        def last_d2d(t):
            got(b_land, sem_re.at[2, t], h)
            got(b_land, sem_re.at[3, t], h)
            remote(land(b_land, 3, t), land(b_land, 7, t), sem_sd.at[3, t], sem_rd.at[3, t], mate).start()

        at_lag(q, 6, last_d2d)

        def load(t):
            got(a_land, sem_ra.at[2, t], h)
            got(a_land, sem_ra.at[3, t], h)
            for k in range(4):
                got(b_land, sem_rd.at[k, t], ch)
            slot = t % 2
            for c in local_loads(t, slot):
                c.start()

            @pl.when(is0)
            def _():
                own_e_load(t, slot, own(b_own, t)).start()

            @pl.when(jnp.logical_not(is0))
            def _():
                own_e_load(t, slot, land(b_land, 0, t)).start()

        at_lag(q, 7, load)

        def multiply(t):
            slot = t % 2
            for c in local_loads(t, slot):
                c.wait()
            own_e_load(t, slot, land(b_land, 0, t)).wait()
            pitch = o_buf.shape[1] // hid
            for c in range(ch):
                rhs = b_buf[slot, c].reshape(cores * rows, nc * cols)
                prod = lax.dot_general(a_buf[slot, c], rhs, (((1,), (1,)), ((), ())), preferred_element_type=F32)
                at = pl.ds(pl.multiple_of((t * ch + c) * pitch, 8), rows)
                for j in range(o_buf.shape[0]):
                    o_buf[j, at, :] = prod[:, j * 128:(j + 1) * 128]

        at_lag(q, 8, multiply)
        return 0

    lax.fori_loop(0, n + 8, step, 0)

    load_z.wait()
    pitch = o_buf.shape[1] // hid

    def back_row(i, _):
        z = z_buf[i].astype(F32)
        xn = normalize(z, g_in[...])
        gate = jax.nn.sigmoid(jnp.dot(w_gate[...], xn, preferred_element_type=F32))
        o = jnp.concatenate([o_buf[j, pl.ds(i, hid, stride=pitch), :] for j in range(o_buf.shape[0])], axis=1)
        on = normalize(o, g_out[...])
        update = jnp.dot(w_out[...], on, preferred_element_type=F32)
        z_buf[i] = (z + gate * update).astype(BF16)
        return 0

    per = rows // 8
    for blk in range(8):
        lax.fori_loop(blk * per, (blk + 1) * per, back_row, 0, unroll=2)
        pltpu.make_async_copy(z_buf.at[pl.ds(blk * per, per)], out_hbm.at[pl.ds(blk * per, per)], sem_z.at[1 + blk]).start()

    def drain(t, _):
        for k in range(4):
            pltpu.make_async_copy(own(b_own, t, h), own(b_own, t, h), sem_sp.at[k, t]).wait()
            pltpu.make_async_copy(own(b_own, t), own(b_own, t), sem_sd.at[k, t]).wait()
        for k in range(4):
            cnt = ch if k < 2 else h
            pltpu.make_async_copy(own(b_own, t, cnt), own(b_own, t, cnt), sem_sa.at[k, t]).wait()
            pltpu.make_async_copy(own(b_own, t, cnt), own(b_own, t, cnt), sem_se.at[k, t]).wait()
        return 0

    lax.fori_loop(0, n, drain, 0)
    for blk in range(8):
        pltpu.make_async_copy(z_buf.at[pl.ds(blk * per, per)], out_hbm.at[pl.ds(blk * per, per)], sem_z.at[1 + blk]).wait()


def main_call(nc, a_own, b_own, z_t, g_in, w_gate, g_out, w_out):
    hid, rows, cols = a_own.shape
    chan = z_t.shape[1]
    ch = 2 * PER_HALF
    n = hid // ch
    any_spec = pl.BlockSpec(memory_space=pl.ANY)
    vm = pl.BlockSpec(memory_space=pltpu.VMEM)
    dma = lambda *s: pltpu.SemaphoreType.DMA(s)
    return pl.pallas_call(
        functools.partial(main_kernel, nc),
        in_specs=[any_spec] * 3 + [vm] * 4,
        out_specs=[any_spec] * 3,
        out_shape=[
            jax.ShapeDtypeStruct(z_t.shape, BF16),
            jax.ShapeDtypeStruct((3 * hid, rows, cols), BF16),
            jax.ShapeDtypeStruct((10 * hid, rows, cols), BF16),
        ],
        scratch_shapes=[
            pltpu.VMEM((2, ch, rows, nc * cols), BF16),
            pltpu.VMEM((2, ch, 2, rows, nc * cols), BF16),
            pltpu.VMEM((cols // 128, hid * (rows + 8), 128), F32),
            pltpu.VMEM(z_t.shape, BF16),
            dma(4, n), dma(6, n), dma(4, n), dma(4, n), dma(4, n), dma(4, n), dma(4, n), dma(4, n),
            dma(2, 12), dma(9),
        ],
        compiler_params=pltpu.CompilerParams(
            vmem_limit_bytes=VMEM_LIMIT, collective_id=0, has_side_effects=True),
        name="exchange",
    )(a_own, b_own, z_t, g_in, w_gate, g_out, w_out)[0]


def solution(mesh):
    nc = mesh.shape['col']
    tile_spec = P(('dp', 'row'), 'col', None)
    mask_spec = P(('dp', 'row'), 'col')

    def tile_program(pair_tile, mask_tile, norm_in, proj_left, gate_left, proj_right, gate_right, proj_gate, norm_out, proj_out):
        z_t = jnp.transpose(pair_tile, (0, 2, 1))
        w_cat = jnp.concatenate([proj_left, gate_left, proj_right, gate_right], axis=1).T
        g_in = norm_in.astype(F32)[:, None]
        g_out = norm_out.astype(F32)[:, None]
        a_own, b_own = front(z_t, mask_tile, g_in, w_cat)
        out = main_call(nc, a_own, b_own, z_t, g_in, proj_gate.T, g_out, proj_out.T)
        return jnp.transpose(out, (0, 2, 1))

    return jax.shard_map(tile_program, mesh=mesh, in_specs=(tile_spec, mask_spec) + (P(),) * 8, out_specs=tile_spec, check_vma=False)
```

```python
import functools

import jax
import jax.numpy as jnp
from jax import lax
from jax.experimental import pallas as pl
from jax.experimental.pallas import tpu as pltpu
from jax.sharding import PartitionSpec as P

LN_EPS = 1e-5
F32 = jnp.float32
BF16 = jnp.bfloat16
MESH = pl.DeviceIdType.MESH
VMEM_LIMIT = 66_000_000
PER_HALF = 1
GROUP = 8
BLOCK = 16


def normalize(values, gain):
    centre = values - jnp.mean(values, axis=0, keepdims=True)
    spread = jnp.mean(centre * centre, axis=0, keepdims=True)
    return (centre * lax.rsqrt(spread + LN_EPS) * gain).astype(BF16)


def main_kernel(nc, z_hbm, mask, norm_in, proj_left, gate_left, proj_right, gate_right, proj_gate, norm_out,
                proj_out, out_hbm, a_own, b_own, a_land, b_land,
                a_buf, b_buf, o_buf, z_buf, s_buf, stage_a, stage_b, turn, w_front, w_gate, w_out, g_in, g_out, sem_sp, sem_rp, sem_sa, sem_ra, sem_se, sem_re,
                sem_sd, sem_rd, sem_l, sem_z, sem_in, sem_st):
    hid, rows, cols = a_own.shape
    h = PER_HALF
    ch = 2 * h
    n = hid // ch
    half = hid // 2
    relay0 = 8 * hid
    dp, y, r = lax.axis_index("dp"), lax.axis_index("col"), lax.axis_index("row")
    cores = 2
    x, core = r // cores, r % cores
    up = lambda v: (v + 1) % nc
    dn = lambda v: (v + nc - 1) % nc
    xp, xm = (dp, y, up(x) * cores + core), (dp, y, dn(x) * cores + core)
    yp, ym = (dp, up(y), r), (dp, dn(y), r)
    mate = (dp, y, x * cores + 1 - core)
    cls = (y + nc - x) % nc
    is0 = cls == 0
    eq = [(cls == k).astype(jnp.int32) for k in range(4)]
    pick = lambda c0, c1, c2, c3: eq[0] * c0 + eq[1] * c1 + eq[2] * c2 + eq[3] * c3

    barrier = pltpu.get_barrier_semaphore()
    for dev in (xp, xm, yp, ym, mate):
        pl.semaphore_signal(barrier, inc=1, device_id=dev, device_id_type=MESH)

    parts = GROUP // ch
    part_rows = rows // parts
    groups = hid // GROUP
    tiles = cols // 128
    turn_pitch = turn.shape[1] // BLOCK

    def first_load(p):
        at = pl.ds(p * part_rows, part_rows)
        return pltpu.make_async_copy(z_hbm.at[at], z_buf.at[at], sem_in.at[p])

    for p in range(parts):
        first_load(p).start()
    for k, w in enumerate((proj_left, gate_left, proj_right, gate_right)):
        w_t = w[...].astype(F32).T
        for g in range(groups):
            w_front[g, k * GROUP:(k + 1) * GROUP, :] = w_t[g * GROUP:(g + 1) * GROUP]
    w_gate[...] = proj_gate[...].astype(F32).T.astype(BF16)
    w_out[...] = proj_out[...].astype(F32).T.astype(BF16)
    g_in[...] = jnp.broadcast_to(norm_in[...].astype(F32), (g_in.shape[0], g_in.shape[0])).T
    g_out[...] = jnp.broadcast_to(norm_out[...].astype(F32), (g_out.shape[0], g_out.shape[0])).T

    def front_part(g, p, first=False):
        w = w_front[g].astype(BF16)

        def block(blk, _):
            def row(i, _):
                r_i = blk * BLOCK + i
                xn = z_buf[r_i]
                if first:
                    xn = normalize(xn.astype(F32), g_in[:, :1])
                    z_buf[r_i] = xn
                v = jnp.dot(w, xn, preferred_element_type=F32)
                keep = mask[pl.ds(r_i, 1), :].astype(F32)
                left = keep * jax.nn.sigmoid(v[GROUP:2 * GROUP]) * v[:GROUP]
                right = keep * jax.nn.sigmoid(v[3 * GROUP:]) * v[2 * GROUP:3 * GROUP]
                at = pl.multiple_of(i * turn_pitch, 8)
                for j in range(tiles):
                    turn[j, pl.ds(at, GROUP), :] = left[:, j * 128:(j + 1) * 128]
                    turn[j, pl.ds(at + GROUP, GROUP), :] = right[:, j * 128:(j + 1) * 128]
                return 0

            lax.fori_loop(0, BLOCK, row, 0, unroll=4)
            to = pl.ds(pl.multiple_of(blk * BLOCK, BLOCK), BLOCK)
            for c in range(GROUP):
                for j in range(tiles):
                    at = slice(j * 128, (j + 1) * 128)
                    stage_a[g % 2, c, to, at] = turn[j, pl.ds(c, BLOCK, stride=turn_pitch), :].astype(BF16)
                    stage_b[g % 2, c, to, at] = turn[j, pl.ds(GROUP + c, BLOCK, stride=turn_pitch), :].astype(BF16)
            return 0

        per = part_rows // BLOCK
        lax.fori_loop(p * per, (p + 1) * per, block, 0)

    def stage_out(g):
        to = pl.ds(g * GROUP, GROUP)
        return [
            pltpu.make_async_copy(stage_a.at[g % 2], a_own.at[to], sem_st.at[0, g % 2]),
            pltpu.make_async_copy(stage_b.at[g % 2], b_own.at[to], sem_st.at[1, g % 2]),
        ]

    for p in range(parts):
        first_load(p).wait()
        front_part(0, p, first=True)
    for c in stage_out(0):
        c.start()
    pl.semaphore_wait(barrier, 5)

    dirs = [pick(1, 3, 0, 2), pick(0, 1, 1, 0), pick(2, 0, 3, 1), pick(3, 2, 2, 3)]
    hops = [pick(2, 1, 1, 1), pick(2, 1, 1, 1), pick(3, 2, 2, 2), pick(3, 4, 2, 4)]
    src_relay = [3, 2, pick(0, 0, 1, 1), pick(1, 2, 0, 3)]
    tgt = [pick(4, 3, 0, 2), pick(4, 1, 1, 0), pick(2, 0, 5, 1), pick(3, 4, 5, 5)]

    def dev_of(d):
        dx = (d == 0).astype(jnp.int32) + 3 * (d == 1).astype(jnp.int32)
        dy = (d == 2).astype(jnp.int32) + 3 * (d == 3).astype(jnp.int32)
        return (dp, (y + dy) % nc, ((x + dx) % nc) * cores + core)

    perm_devs = [dev_of(d) for d in dirs]

    def tgt_at(k, t):
        to_e = tgt[k] // 4
        return (1 - to_e) * (relay0 + tgt[k] * half + t * h) + to_e * ((2 * t + tgt[k] - 4) * h)

    def remote(src, dst, send, recv, dev):
        return pltpu.make_async_remote_copy(src_ref=src, dst_ref=dst, send_sem=send, recv_sem=recv,
                                            device_id=dev, device_id_type=MESH)

    def perm_copy(k, t, src):
        return remote(src, b_land.at[pl.ds(tgt_at(k, t), h)], sem_sp.at[k, t], sem_rp.at[tgt[k], t], perm_devs[k])

    def got_perm(which, t):
        pltpu.make_async_copy(b_land.at[pl.ds(0, h)], b_land.at[pl.ds(0, h)], sem_rp.at[which, t]).wait()

    def land(buf, slot, t, f=0, count=ch):
        return buf.at[pl.ds(slot * hid + t * ch + f * h, count)]

    def got(buf, sem, count):
        pltpu.make_async_copy(buf.at[pl.ds(0, count)], buf.at[pl.ds(0, count)], sem).wait()

    def own(buf, t, count=ch, f=0):
        return buf.at[pl.ds(t * ch + f * h, count)]

    def a_own_sends(t):
        return [
            remote(own(a_own, t), land(a_land, 0, t), sem_sa.at[0, t], sem_ra.at[0, t], yp),
            remote(own(a_own, t), land(a_land, 1, t), sem_sa.at[1, t], sem_ra.at[1, t], ym),
        ]

    def e_own_sends(t, src):
        return [
            remote(src, land(b_land, 1, t), sem_se.at[0, t], sem_re.at[0, t], xp),
            remote(src, land(b_land, 2, t), sem_se.at[1, t], sem_re.at[1, t], xm),
            remote(src, land(b_land, 4, t), sem_sd.at[0, t], sem_rd.at[0, t], mate),
        ]

    def local_loads(t, slot):
        put_a = lambda rel: a_buf.at[slot, :, :, pl.ds(rel * cols, cols)]
        out = [
            (own(a_own, t), put_a(0)),
            (land(a_land, 0, t), put_a(3)),
            (land(a_land, 1, t), put_a(1)),
            (land(a_land, 2, t), put_a(2)),
        ]
        for k, delta in enumerate((0, 3, 1, 2)):
            rel = (cls + nc - delta) % nc
            where = pl.ds(pl.multiple_of(rel * cols, 128), cols)
            if k > 0:
                out.append((land(b_land, k, t), b_buf.at[slot, :, core, :, where]))
            out.append((land(b_land, 4 + k, t), b_buf.at[slot, :, 1 - core, :, where]))
        return [pltpu.make_async_copy(s, d, sem_l.at[slot, j]) for j, (s, d) in enumerate(out)]

    def own_e_load(t, slot, src):
        where = pl.ds(pl.multiple_of(cls * cols, 128), cols)
        return pltpu.make_async_copy(src, b_buf.at[slot, :, core, :, where], sem_l.at[slot, 11])

    def at_lag(q, lag, fn):
        t = q - lag

        @pl.when(jnp.logical_and(t >= 0, t < n))
        def _():
            fn(t)

    gate_rows = rows // (n - 2 * parts)

    def gate_row(first, j, _):
        i = first + j
        s_buf[i] = jax.nn.sigmoid(jnp.dot(w_gate[...], z_buf[i], preferred_element_type=F32))
        return 0

    def step(q, _):
        @pl.when(jnp.logical_and(q < n, q % parts == 0))
        def _():
            for c in stage_out(q // parts):
                c.wait()

        for k in range(4):
            def send(t, k=k):
                if k < 2:
                    @pl.when(is0)
                    def _():
                        got_perm(src_relay[k], t)
                        perm_copy(k, t, b_land.at[pl.ds(relay0 + src_relay[k] * half + t * h, h)]).start()

                    @pl.when(jnp.logical_not(is0))
                    def _():
                        perm_copy(k, t, own(b_own, t, h, k)).start()
                else:
                    got_perm(src_relay[k], t)
                    perm_copy(k, t, b_land.at[pl.ds(relay0 + src_relay[k] * half + t * h, h)]).start()

            at_lag(q, hops[k] - 1, send)

        def e_own(t):
            @pl.when(is0)
            def _():
                for c in e_own_sends(t, own(b_own, t)):
                    c.start()

            @pl.when(jnp.logical_not(is0))
            def _():
                got_perm(4, t)
                got_perm(5, t)
                for c in e_own_sends(t, land(b_land, 0, t)):
                    c.start()

        at_lag(q, 4, e_own)

        def a_first(t):
            for c in a_own_sends(t):
                c.start()

        at_lag(q, 3, a_first)

        def e_fwd(t):
            got(b_land, sem_re.at[0, t], ch)
            remote(land(b_land, 1, t, 0, h), land(b_land, 3, t, 0, h), sem_se.at[2, t], sem_re.at[2, t], xp).start()
            remote(land(b_land, 1, t), land(b_land, 5, t), sem_sd.at[1, t], sem_rd.at[1, t], mate).start()
            got(b_land, sem_re.at[1, t], ch)
            remote(land(b_land, 2, t, 1, h), land(b_land, 3, t, 1, h), sem_se.at[3, t], sem_re.at[3, t], xm).start()
            remote(land(b_land, 2, t), land(b_land, 6, t), sem_sd.at[2, t], sem_rd.at[2, t], mate).start()

        at_lag(q, 5, e_fwd)

        def a_fwd(t):
            got(a_land, sem_ra.at[0, t], ch)
            remote(land(a_land, 0, t, 0, h), land(a_land, 2, t, 0, h), sem_sa.at[2, t], sem_ra.at[2, t], yp).start()
            got(a_land, sem_ra.at[1, t], ch)
            remote(land(a_land, 1, t, 1, h), land(a_land, 2, t, 1, h), sem_sa.at[3, t], sem_ra.at[3, t], ym).start()

        at_lag(q, 4, a_fwd)

        def last_d2d(t):
            got(b_land, sem_re.at[2, t], h)
            got(b_land, sem_re.at[3, t], h)
            remote(land(b_land, 3, t), land(b_land, 7, t), sem_sd.at[3, t], sem_rd.at[3, t], mate).start()

        at_lag(q, 6, last_d2d)

        def load(t):
            got(a_land, sem_ra.at[2, t], h)
            got(a_land, sem_ra.at[3, t], h)
            for k in range(4):
                got(b_land, sem_rd.at[k, t], ch)
            slot = t % 2
            for c in local_loads(t, slot):
                c.start()

            @pl.when(is0)
            def _():
                own_e_load(t, slot, own(b_own, t)).start()

            @pl.when(jnp.logical_not(is0))
            def _():
                own_e_load(t, slot, land(b_land, 0, t)).start()

        at_lag(q, 7, load)

        def multiply(t):
            slot = t % 2
            for c in local_loads(t, slot):
                c.wait()
            own_e_load(t, slot, land(b_land, 0, t)).wait()
            pitch = o_buf.shape[1] // hid
            for c in range(ch):
                rhs = b_buf[slot, c].reshape(cores * rows, nc * cols)
                prod = lax.dot_general(a_buf[slot, c], rhs, (((1,), (1,)), ((), ())), preferred_element_type=F32)
                at = pl.ds(pl.multiple_of((t * ch + c) * pitch, 8), rows)
                for j in range(o_buf.shape[0]):
                    o_buf[j, at, :] = prod[:, j * 128:(j + 1) * 128]

        at_lag(q, 8, multiply)

        @pl.when(q < n - parts)
        def _():
            front_part(q // parts + 1, q % parts)

            @pl.when(q % parts == parts - 1)
            def _():
                for c in stage_out(q // parts + 1):
                    c.start()

        @pl.when(q < n - 2 * parts)
        def _():
            lax.fori_loop(0, gate_rows, functools.partial(gate_row, q * gate_rows), 0, unroll=4)

        @pl.when(q == n - parts)
        def _():
            pltpu.make_async_copy(z_hbm, z_buf, sem_z.at[0]).start()

        return 0

    lax.fori_loop(0, n + 8, step, 0)

    pltpu.make_async_copy(z_hbm, z_buf, sem_z.at[0]).wait()
    pitch = o_buf.shape[1] // hid

    def back_row(i, _):
        o = jnp.concatenate([o_buf[j, pl.ds(i, hid, stride=pitch), :] for j in range(o_buf.shape[0])], axis=1)
        on = normalize(o, g_out[:, :1])
        update = jnp.dot(w_out[...], on, preferred_element_type=F32)
        z_buf[i] = (z_buf[i].astype(F32) + s_buf[i] * update).astype(BF16)
        return 0

    per = rows // 8
    for blk in range(8):
        lax.fori_loop(blk * per, (blk + 1) * per, back_row, 0, unroll=2)
        pltpu.make_async_copy(z_buf.at[pl.ds(blk * per, per)], out_hbm.at[pl.ds(blk * per, per)], sem_z.at[1 + blk]).start()

    def drain(t, _):
        for k in range(4):
            pltpu.make_async_copy(own(b_own, t, h), own(b_own, t, h), sem_sp.at[k, t]).wait()
            pltpu.make_async_copy(own(b_own, t), own(b_own, t), sem_sd.at[k, t]).wait()
        for k in range(4):
            cnt = ch if k < 2 else h
            pltpu.make_async_copy(own(b_own, t, cnt), own(b_own, t, cnt), sem_sa.at[k, t]).wait()
            pltpu.make_async_copy(own(b_own, t, cnt), own(b_own, t, cnt), sem_se.at[k, t]).wait()
        return 0

    lax.fori_loop(0, n, drain, 0)
    for blk in range(8):
        pltpu.make_async_copy(z_buf.at[pl.ds(blk * per, per)], out_hbm.at[pl.ds(blk * per, per)], sem_z.at[1 + blk]).wait()


def main_call(nc, z_t, mask, small):
    rows, chan, cols = z_t.shape
    hid = chan
    ch = 2 * PER_HALF
    n = hid // ch
    any_spec = pl.BlockSpec(memory_space=pl.ANY)
    vm = pl.BlockSpec(memory_space=pltpu.VMEM)
    dma = lambda *s: pltpu.SemaphoreType.DMA(s)
    return pl.pallas_call(
        functools.partial(main_kernel, nc),
        in_specs=[any_spec] + [vm] * (1 + len(small)),
        out_specs=[any_spec] * 5,
        out_shape=[
            jax.ShapeDtypeStruct(z_t.shape, BF16),
            jax.ShapeDtypeStruct((hid, rows, cols), BF16),
            jax.ShapeDtypeStruct((hid, rows, cols), BF16),
            jax.ShapeDtypeStruct((3 * hid, rows, cols), BF16),
            jax.ShapeDtypeStruct((10 * hid, rows, cols), BF16),
        ],
        scratch_shapes=[
            pltpu.VMEM((2, ch, rows, nc * cols), BF16),
            pltpu.VMEM((2, ch, 2, rows, nc * cols), BF16),
            pltpu.VMEM((cols // 128, hid * (rows + 8), 128), F32),
            pltpu.VMEM(z_t.shape, BF16),
            pltpu.VMEM(z_t.shape, F32),
            pltpu.VMEM((2, GROUP, rows, cols), BF16),
            pltpu.VMEM((2, GROUP, rows, cols), BF16),
            pltpu.VMEM((cols // 128, BLOCK * (2 * GROUP + 8), 128), F32),
            pltpu.VMEM((hid // GROUP, 4 * GROUP, chan), F32),
            pltpu.VMEM((chan, chan), BF16),
            pltpu.VMEM((chan, hid), BF16),
            pltpu.VMEM((chan, chan), F32),
            pltpu.VMEM((hid, hid), F32),
            dma(4, n), dma(6, n), dma(4, n), dma(4, n), dma(4, n), dma(4, n), dma(4, n), dma(4, n),
            dma(2, 12), dma(9), dma(GROUP // ch), dma(2, 2),
        ],
        compiler_params=pltpu.CompilerParams(
            vmem_limit_bytes=VMEM_LIMIT, collective_id=0, has_side_effects=True),
        name="exchange",
    )(z_t, mask, *small)[0]


def solution(mesh):
    nc = mesh.shape['col']
    tile_spec = P(('dp', 'row'), 'col', None)
    mask_spec = P(('dp', 'row'), 'col')

    def tile_program(pair_tile, mask_tile, norm_in, proj_left, gate_left, proj_right, gate_right, proj_gate, norm_out, proj_out):
        z_t = jnp.transpose(pair_tile, (0, 2, 1))
        small = (norm_in[None, :], proj_left, gate_left, proj_right, gate_right, proj_gate, norm_out[None, :], proj_out)
        return jnp.transpose(main_call(nc, z_t, mask_tile, small), (0, 2, 1))

    return jax.shard_map(tile_program, mesh=mesh, in_specs=(tile_spec, mask_spec) + (P(),) * 8, out_specs=tile_spec, check_vma=False)
```

```python
import functools

import jax
import jax.numpy as jnp
from jax import lax
from jax.experimental import pallas as pl
from jax.experimental.pallas import tpu as pltpu
from jax.sharding import PartitionSpec as P

LN_EPS = 1e-5
F32 = jnp.float32
BF16 = jnp.bfloat16
MESH = pl.DeviceIdType.MESH
VMEM_LIMIT = 66_000_000
PER_HALF = 1
GROUP = 8
BLOCK = 16
FRONT_UNROLL = 16
BACK_UNROLL = 12
LEAD = 4


def normalize(values, gain):
    centre = values - jnp.mean(values, axis=0, keepdims=True)
    spread = jnp.mean(centre * centre, axis=0, keepdims=True)
    return (centre * lax.rsqrt(spread + LN_EPS) * gain).astype(BF16)


def main_kernel(nc, z_hbm, mask, norm_in, proj_left, gate_left, proj_right, gate_right, proj_gate, norm_out,
                proj_out, out_hbm, a_own, b_own, a_land, b_land,
                a_buf, b_buf, o_buf, z_buf, s_buf, stage_a, stage_b, turn, w_front, w_gate, w_out, g_in, g_out, sem_sp, sem_rp, sem_sa, sem_ra, sem_se, sem_re,
                sem_sd, sem_rd, sem_l, sem_z, sem_in, sem_st):
    hid, rows, cols = a_own.shape
    h = PER_HALF
    ch = 2 * h
    n = hid // ch
    half = hid // 2
    relay0 = 8 * hid
    dp, y, r = lax.axis_index("dp"), lax.axis_index("col"), lax.axis_index("row")
    cores = 2
    x, core = r // cores, r % cores
    up = lambda v: (v + 1) % nc
    dn = lambda v: (v + nc - 1) % nc
    xp, xm = (dp, y, up(x) * cores + core), (dp, y, dn(x) * cores + core)
    yp, ym = (dp, up(y), r), (dp, dn(y), r)
    mate = (dp, y, x * cores + 1 - core)
    cls = (y + nc - x) % nc
    is0 = cls == 0
    eq = [(cls == k).astype(jnp.int32) for k in range(4)]
    pick = lambda c0, c1, c2, c3: eq[0] * c0 + eq[1] * c1 + eq[2] * c2 + eq[3] * c3

    barrier = pltpu.get_barrier_semaphore()
    for dev in (xp, xm, yp, ym, mate):
        pl.semaphore_signal(barrier, inc=1, device_id=dev, device_id_type=MESH)

    parts = GROUP // ch
    part_rows = rows // parts
    groups = hid // GROUP
    tiles = cols // 128
    turn_pitch = turn.shape[1] // BLOCK

    def first_load(p):
        at = pl.ds(p * part_rows, part_rows)
        return pltpu.make_async_copy(z_hbm.at[at], z_buf.at[at], sem_in.at[p])

    for p in range(parts):
        first_load(p).start()
    for k, w in enumerate((proj_left, gate_left, proj_right, gate_right)):
        w_t = w[...].astype(F32).T
        for g in range(groups):
            w_front[g, k * GROUP:(k + 1) * GROUP, :] = w_t[g * GROUP:(g + 1) * GROUP]
    w_gate[...] = proj_gate[...].astype(F32).T.astype(BF16)
    w_out[...] = proj_out[...].astype(F32).T.astype(BF16)
    g_in[...] = jnp.broadcast_to(norm_in[...].astype(F32), (g_in.shape[0], g_in.shape[0])).T
    g_out[...] = jnp.broadcast_to(norm_out[...].astype(F32), (g_out.shape[0], g_out.shape[0])).T

    def front_part(g, p, first=False):
        w = w_front[g].astype(BF16)

        def block(blk, _):
            def row(i, _):
                r_i = blk * BLOCK + i
                xn = z_buf[r_i]
                if first:
                    xn = normalize(xn.astype(F32), g_in[:, :1])
                    z_buf[r_i] = xn
                v = jnp.dot(w, xn, preferred_element_type=F32)
                keep = mask[pl.ds(r_i, 1), :].astype(F32)
                left = keep * jax.nn.sigmoid(v[GROUP:2 * GROUP]) * v[:GROUP]
                right = keep * jax.nn.sigmoid(v[3 * GROUP:]) * v[2 * GROUP:3 * GROUP]
                at = pl.multiple_of(i * turn_pitch, 8)
                for j in range(tiles):
                    turn[j, pl.ds(at, GROUP), :] = left[:, j * 128:(j + 1) * 128]
                    turn[j, pl.ds(at + GROUP, GROUP), :] = right[:, j * 128:(j + 1) * 128]
                return 0

            lax.fori_loop(0, BLOCK, row, 0, unroll=FRONT_UNROLL)
            to = pl.ds(pl.multiple_of(blk * BLOCK, BLOCK), BLOCK)
            for c in range(GROUP):
                for j in range(tiles):
                    at = slice(j * 128, (j + 1) * 128)
                    stage_a[g % 2, c, to, at] = turn[j, pl.ds(c, BLOCK, stride=turn_pitch), :].astype(BF16)
                    stage_b[g % 2, c, to, at] = turn[j, pl.ds(GROUP + c, BLOCK, stride=turn_pitch), :].astype(BF16)
            return 0

        per = part_rows // BLOCK
        lax.fori_loop(p * per, (p + 1) * per, block, 0)

    def stage_out(g):
        to = pl.ds(g * GROUP, GROUP)
        return [
            pltpu.make_async_copy(stage_a.at[g % 2], a_own.at[to], sem_st.at[0, g % 2]),
            pltpu.make_async_copy(stage_b.at[g % 2], b_own.at[to], sem_st.at[1, g % 2]),
        ]

    for p in range(parts):
        first_load(p).wait()
        front_part(0, p, first=True)
    for c in stage_out(0):
        c.start()
    pl.semaphore_wait(barrier, 5)

    dirs = [pick(1, 3, 0, 2), pick(0, 1, 1, 0), pick(2, 0, 3, 1), pick(3, 2, 2, 3)]
    hops = [pick(2, 1, 1, 1), pick(2, 1, 1, 1), pick(3, 2, 2, 2), pick(3, 4, 2, 4)]
    src_relay = [3, 2, pick(0, 0, 1, 1), pick(1, 2, 0, 3)]
    tgt = [pick(4, 3, 0, 2), pick(4, 1, 1, 0), pick(2, 0, 5, 1), pick(3, 4, 5, 5)]

    def dev_of(d):
        dx = (d == 0).astype(jnp.int32) + 3 * (d == 1).astype(jnp.int32)
        dy = (d == 2).astype(jnp.int32) + 3 * (d == 3).astype(jnp.int32)
        return (dp, (y + dy) % nc, ((x + dx) % nc) * cores + core)

    perm_devs = [dev_of(d) for d in dirs]

    def tgt_at(k, t):
        to_e = tgt[k] // 4
        return (1 - to_e) * (relay0 + tgt[k] * half + t * h) + to_e * ((2 * t + tgt[k] - 4) * h)

    def remote(src, dst, send, recv, dev):
        return pltpu.make_async_remote_copy(src_ref=src, dst_ref=dst, send_sem=send, recv_sem=recv,
                                            device_id=dev, device_id_type=MESH)

    def perm_copy(k, t, src):
        return remote(src, b_land.at[pl.ds(tgt_at(k, t), h)], sem_sp.at[k, t], sem_rp.at[tgt[k], t], perm_devs[k])

    def got_perm(which, t):
        pltpu.make_async_copy(b_land.at[pl.ds(0, h)], b_land.at[pl.ds(0, h)], sem_rp.at[which, t]).wait()

    def land(buf, slot, t, f=0, count=ch):
        return buf.at[pl.ds(slot * hid + t * ch + f * h, count)]

    def got(buf, sem, count):
        pltpu.make_async_copy(buf.at[pl.ds(0, count)], buf.at[pl.ds(0, count)], sem).wait()

    def own(buf, t, count=ch, f=0):
        return buf.at[pl.ds(t * ch + f * h, count)]

    def a_own_sends(t):
        return [
            remote(own(a_own, t), land(a_land, 0, t), sem_sa.at[0, t], sem_ra.at[0, t], yp),
            remote(own(a_own, t), land(a_land, 1, t), sem_sa.at[1, t], sem_ra.at[1, t], ym),
        ]

    def e_own_sends(t, src):
        return [
            remote(src, land(b_land, 1, t), sem_se.at[0, t], sem_re.at[0, t], xp),
            remote(src, land(b_land, 2, t), sem_se.at[1, t], sem_re.at[1, t], xm),
            remote(src, land(b_land, 4, t), sem_sd.at[0, t], sem_rd.at[0, t], mate),
        ]

    def local_loads(t, slot):
        put_a = lambda rel: a_buf.at[slot, :, :, pl.ds(rel * cols, cols)]
        out = [
            (own(a_own, t), put_a(0)),
            (land(a_land, 0, t), put_a(3)),
            (land(a_land, 1, t), put_a(1)),
            (land(a_land, 2, t), put_a(2)),
        ]
        for k, delta in enumerate((0, 3, 1, 2)):
            rel = (cls + nc - delta) % nc
            where = pl.ds(pl.multiple_of(rel * cols, 128), cols)
            if k > 0:
                out.append((land(b_land, k, t), b_buf.at[slot, :, core, :, where]))
            out.append((land(b_land, 4 + k, t), b_buf.at[slot, :, 1 - core, :, where]))
        return [pltpu.make_async_copy(s, d, sem_l.at[slot, j]) for j, (s, d) in enumerate(out)]

    def own_e_load(t, slot, src):
        where = pl.ds(pl.multiple_of(cls * cols, 128), cols)
        return pltpu.make_async_copy(src, b_buf.at[slot, :, core, :, where], sem_l.at[slot, 11])

    def at_lag(q, lag, fn):
        t = q - lag

        @pl.when(jnp.logical_and(t >= 0, t < n))
        def _():
            fn(t)

    gate_rows = rows // (n - 2 * parts)

    def gate_row(first, j, _):
        i = first + j
        s_buf[i] = jax.nn.sigmoid(jnp.dot(w_gate[...], z_buf[i], preferred_element_type=F32))
        return 0

    def drain(t):
        for k in range(4):
            pltpu.make_async_copy(own(b_own, t, h), own(b_own, t, h), sem_sp.at[k, t]).wait()
            pltpu.make_async_copy(own(b_own, t), own(b_own, t), sem_sd.at[k, t]).wait()
        for k in range(4):
            cnt = ch if k < 2 else h
            pltpu.make_async_copy(own(b_own, t, cnt), own(b_own, t, cnt), sem_sa.at[k, t]).wait()
            pltpu.make_async_copy(own(b_own, t, cnt), own(b_own, t, cnt), sem_se.at[k, t]).wait()

    def perm_step(v):
        @pl.when(jnp.logical_and(v < n, v % parts == 0))
        def _():
            for c in stage_out(v // parts):
                c.wait()

        for k in range(4):
            def send(t, k=k):
                if k < 2:
                    @pl.when(is0)
                    def _():
                        got_perm(src_relay[k], t)
                        perm_copy(k, t, b_land.at[pl.ds(relay0 + src_relay[k] * half + t * h, h)]).start()

                    @pl.when(jnp.logical_not(is0))
                    def _():
                        perm_copy(k, t, own(b_own, t, h, k)).start()
                else:
                    got_perm(src_relay[k], t)
                    perm_copy(k, t, b_land.at[pl.ds(relay0 + src_relay[k] * half + t * h, h)]).start()

            at_lag(v, hops[k] - 1, send)

    def front_step(v):
        @pl.when(v < n - parts)
        def _():
            front_part(v // parts + 1, v % parts)

            @pl.when(v % parts == parts - 1)
            def _():
                for c in stage_out(v // parts + 1):
                    c.start()

    def step(q, _):
        early = q < LEAD
        v0 = jnp.where(early, 2 * q, q + LEAD)
        perm_step(v0)

        @pl.when(early)
        def _():
            front_step(2 * q)
            perm_step(2 * q + 1)

        def e_own(t):
            @pl.when(is0)
            def _():
                for c in e_own_sends(t, own(b_own, t)):
                    c.start()

            @pl.when(jnp.logical_not(is0))
            def _():
                got_perm(4, t)
                got_perm(5, t)
                for c in e_own_sends(t, land(b_land, 0, t)):
                    c.start()

        at_lag(q, 2, e_own)

        def a_first(t):
            for c in a_own_sends(t):
                c.start()

        at_lag(q, 2, a_first)

        def e_fwd(t):
            got(b_land, sem_re.at[0, t], ch)
            remote(land(b_land, 1, t, 0, h), land(b_land, 3, t, 0, h), sem_se.at[2, t], sem_re.at[2, t], xp).start()
            remote(land(b_land, 1, t), land(b_land, 5, t), sem_sd.at[1, t], sem_rd.at[1, t], mate).start()
            got(b_land, sem_re.at[1, t], ch)
            remote(land(b_land, 2, t, 1, h), land(b_land, 3, t, 1, h), sem_se.at[3, t], sem_re.at[3, t], xm).start()
            remote(land(b_land, 2, t), land(b_land, 6, t), sem_sd.at[2, t], sem_rd.at[2, t], mate).start()

        at_lag(q, 5, e_fwd)

        def a_fwd(t):
            got(a_land, sem_ra.at[0, t], ch)
            remote(land(a_land, 0, t, 0, h), land(a_land, 2, t, 0, h), sem_sa.at[2, t], sem_ra.at[2, t], yp).start()
            got(a_land, sem_ra.at[1, t], ch)
            remote(land(a_land, 1, t, 1, h), land(a_land, 2, t, 1, h), sem_sa.at[3, t], sem_ra.at[3, t], ym).start()

        at_lag(q, 5, a_fwd)

        def last_d2d(t):
            got(b_land, sem_re.at[2, t], h)
            got(b_land, sem_re.at[3, t], h)
            remote(land(b_land, 3, t), land(b_land, 7, t), sem_sd.at[3, t], sem_rd.at[3, t], mate).start()

        at_lag(q, 7, last_d2d)

        def load(t):
            got(a_land, sem_ra.at[2, t], h)
            got(a_land, sem_ra.at[3, t], h)
            for k in range(4):
                got(b_land, sem_rd.at[k, t], ch)
            slot = t % 2
            for c in local_loads(t, slot):
                c.start()

            @pl.when(is0)
            def _():
                own_e_load(t, slot, own(b_own, t)).start()

            @pl.when(jnp.logical_not(is0))
            def _():
                own_e_load(t, slot, land(b_land, 0, t)).start()

        at_lag(q, 8, load)

        def multiply(t):
            slot = t % 2
            for c in local_loads(t, slot):
                c.wait()
            own_e_load(t, slot, land(b_land, 0, t)).wait()
            pitch = o_buf.shape[1] // hid
            for c in range(ch):
                rhs = b_buf[slot, c].reshape(cores * rows, nc * cols)
                prod = lax.dot_general(a_buf[slot, c], rhs, (((1,), (1,)), ((), ())), preferred_element_type=F32)
                at = pl.ds(pl.multiple_of((t * ch + c) * pitch, 8), rows)
                for j in range(o_buf.shape[0]):
                    o_buf[j, at, :] = prod[:, j * 128:(j + 1) * 128]

        at_lag(q, 9, multiply)
        at_lag(q, 9, drain)

        front_step(jnp.where(early, 2 * q + 1, q + LEAD))

        @pl.when(q < n - 2 * parts)
        def _():
            lax.fori_loop(0, gate_rows, functools.partial(gate_row, q * gate_rows), 0, unroll=4)

        @pl.when(q == n - parts)
        def _():
            pltpu.make_async_copy(z_hbm, z_buf, sem_z.at[0]).start()

        return 0

    lax.fori_loop(0, n + 9, step, 0)

    pltpu.make_async_copy(z_hbm, z_buf, sem_z.at[0]).wait()
    pitch = o_buf.shape[1] // hid

    def back_row(i, _):
        o = jnp.concatenate([o_buf[j, pl.ds(i, hid, stride=pitch), :] for j in range(o_buf.shape[0])], axis=1)
        on = normalize(o, g_out[:, :1])
        update = jnp.dot(w_out[...], on, preferred_element_type=F32)
        z_buf[i] = (z_buf[i].astype(F32) + s_buf[i] * update).astype(BF16)
        return 0

    per = rows // 8
    for blk in range(8):
        lax.fori_loop(blk * per, (blk + 1) * per, back_row, 0, unroll=BACK_UNROLL)
        pltpu.make_async_copy(z_buf.at[pl.ds(blk * per, per)], out_hbm.at[pl.ds(blk * per, per)], sem_z.at[1 + blk]).start()

    for blk in range(8):
        pltpu.make_async_copy(z_buf.at[pl.ds(blk * per, per)], out_hbm.at[pl.ds(blk * per, per)], sem_z.at[1 + blk]).wait()


def main_call(nc, z_t, mask, small):
    rows, chan, cols = z_t.shape
    hid = chan
    ch = 2 * PER_HALF
    n = hid // ch
    any_spec = pl.BlockSpec(memory_space=pl.ANY)
    vm = pl.BlockSpec(memory_space=pltpu.VMEM)
    dma = lambda *s: pltpu.SemaphoreType.DMA(s)
    return pl.pallas_call(
        functools.partial(main_kernel, nc),
        in_specs=[any_spec] + [vm] * (1 + len(small)),
        out_specs=[any_spec] * 5,
        out_shape=[
            jax.ShapeDtypeStruct(z_t.shape, BF16),
            jax.ShapeDtypeStruct((hid, rows, cols), BF16),
            jax.ShapeDtypeStruct((hid, rows, cols), BF16),
            jax.ShapeDtypeStruct((3 * hid, rows, cols), BF16),
            jax.ShapeDtypeStruct((10 * hid, rows, cols), BF16),
        ],
        scratch_shapes=[
            pltpu.VMEM((2, ch, rows, nc * cols), BF16),
            pltpu.VMEM((2, ch, 2, rows, nc * cols), BF16),
            pltpu.VMEM((cols // 128, hid * (rows + 8), 128), F32),
            pltpu.VMEM(z_t.shape, BF16),
            pltpu.VMEM(z_t.shape, F32),
            pltpu.VMEM((2, GROUP, rows, cols), BF16),
            pltpu.VMEM((2, GROUP, rows, cols), BF16),
            pltpu.VMEM((cols // 128, BLOCK * (2 * GROUP + 8), 128), F32),
            pltpu.VMEM((hid // GROUP, 4 * GROUP, chan), F32),
            pltpu.VMEM((chan, chan), BF16),
            pltpu.VMEM((chan, hid), BF16),
            pltpu.VMEM((chan, chan), F32),
            pltpu.VMEM((hid, hid), F32),
            dma(4, n), dma(6, n), dma(4, n), dma(4, n), dma(4, n), dma(4, n), dma(4, n), dma(4, n),
            dma(2, 12), dma(9), dma(GROUP // ch), dma(2, 2),
        ],
        compiler_params=pltpu.CompilerParams(
            vmem_limit_bytes=VMEM_LIMIT, collective_id=0, has_side_effects=True),
        name="exchange",
    )(z_t, mask, *small)[0]


def solution(mesh):
    nc = mesh.shape['col']
    tile_spec = P(('dp', 'row'), 'col', None)
    mask_spec = P(('dp', 'row'), 'col')

    def tile_program(pair_tile, mask_tile, norm_in, proj_left, gate_left, proj_right, gate_right, proj_gate, norm_out, proj_out):
        z_t = jnp.transpose(pair_tile, (0, 2, 1))
        small = (norm_in[None, :], proj_left, gate_left, proj_right, gate_right, proj_gate, norm_out[None, :], proj_out)
        return jnp.transpose(main_call(nc, z_t, mask_tile, small), (0, 2, 1))

    return jax.shard_map(tile_program, mesh=mesh, in_specs=(tile_spec, mask_spec) + (P(),) * 8, out_specs=tile_spec, check_vma=False)
```

```python
import functools

import jax
import jax.numpy as jnp
from jax import lax
from jax.experimental import pallas as pl
from jax.experimental.pallas import tpu as pltpu
from jax.sharding import PartitionSpec as P

LN_EPS = 1e-5
F32 = jnp.float32
BF16 = jnp.bfloat16
MESH = pl.DeviceIdType.MESH
VMEM_LIMIT = 66_000_000
PER_HALF = 1
GROUP = 8
BLOCK = 16
FRONT_UNROLL = 16
BACK_UNROLL = 12
LEAD = 4


def normalize(values, gain):
    centre = values - jnp.mean(values, axis=0, keepdims=True)
    spread = jnp.mean(centre * centre, axis=0, keepdims=True)
    return (centre * lax.rsqrt(spread + LN_EPS) * gain).astype(BF16)


def main_kernel(nc, z_hbm, mask, norm_in, proj_left, gate_left, proj_right, gate_right, proj_gate, norm_out,
                proj_out, out_hbm, a_own, b_own, a_land, b_land,
                a_buf, b_buf, o_buf, z_buf, s_buf, stage_a, stage_b, turn, w_front, w_gate, w_out, g_in, g_out, sem_sp, sem_rp, sem_sa, sem_ra, sem_se, sem_re,
                sem_sd, sem_rd, sem_l, sem_z, sem_in, sem_st):
    hid, rows, cols = a_own.shape
    h = PER_HALF
    ch = 2 * h
    n = hid // ch
    half = hid // 2
    relay0 = 8 * hid
    dp, y, r = lax.axis_index("dp"), lax.axis_index("col"), lax.axis_index("row")
    cores = 2
    x, core = r // cores, r % cores
    up = lambda v: (v + 1) % nc
    dn = lambda v: (v + nc - 1) % nc
    xp, xm = (dp, y, up(x) * cores + core), (dp, y, dn(x) * cores + core)
    yp, ym = (dp, up(y), r), (dp, dn(y), r)
    mate = (dp, y, x * cores + 1 - core)
    cls = (y + nc - x) % nc
    is0 = cls == 0
    eq = [(cls == k).astype(jnp.int32) for k in range(4)]
    pick = lambda c0, c1, c2, c3: eq[0] * c0 + eq[1] * c1 + eq[2] * c2 + eq[3] * c3

    barrier = pltpu.get_barrier_semaphore()
    for dev in (xp, xm, yp, ym, mate):
        pl.semaphore_signal(barrier, inc=1, device_id=dev, device_id_type=MESH)

    parts = GROUP // ch
    part_rows = rows // parts
    groups = hid // GROUP
    tiles = cols // 128
    turn_pitch = turn.shape[1] // BLOCK

    def first_load(p):
        at = pl.ds(p * part_rows, part_rows)
        return pltpu.make_async_copy(z_hbm.at[at], z_buf.at[at], sem_in.at[p])

    for p in range(parts):
        first_load(p).start()
    for k, w in enumerate((proj_left, gate_left, proj_right, gate_right)):
        w_t = w[...].astype(F32).T
        for g in range(groups):
            w_front[g, k * GROUP:(k + 1) * GROUP, :] = w_t[g * GROUP:(g + 1) * GROUP]
    w_gate[...] = proj_gate[...].astype(F32).T.astype(BF16)
    w_out[...] = proj_out[...].astype(F32).T.astype(BF16)
    g_in[...] = jnp.broadcast_to(norm_in[...].astype(F32), (g_in.shape[0], g_in.shape[0])).T
    g_out[...] = jnp.broadcast_to(norm_out[...].astype(F32), (g_out.shape[0], g_out.shape[0])).T

    def front_part(g, p, first=False):
        w = w_front[g].astype(BF16)

        def block(blk, _):
            def row(i, _):
                r_i = blk * BLOCK + i
                xn = z_buf[r_i]
                if first:
                    xn = normalize(xn.astype(F32), g_in[:, :1])
                    z_buf[r_i] = xn
                v = jnp.dot(w, xn, preferred_element_type=F32)
                keep = mask[pl.ds(r_i, 1), :].astype(F32)
                left = keep * jax.nn.sigmoid(v[GROUP:2 * GROUP]) * v[:GROUP]
                right = keep * jax.nn.sigmoid(v[3 * GROUP:]) * v[2 * GROUP:3 * GROUP]
                at = pl.multiple_of(i * turn_pitch, 8)
                for j in range(tiles):
                    turn[j, pl.ds(at, GROUP), :] = left[:, j * 128:(j + 1) * 128]
                    turn[j, pl.ds(at + GROUP, GROUP), :] = right[:, j * 128:(j + 1) * 128]
                return 0

            lax.fori_loop(0, BLOCK, row, 0, unroll=FRONT_UNROLL)
            to = pl.ds(pl.multiple_of(blk * BLOCK, BLOCK), BLOCK)
            for c in range(GROUP):
                for j in range(tiles):
                    at = slice(j * 128, (j + 1) * 128)
                    stage_a[g % 2, c, to, at] = turn[j, pl.ds(c, BLOCK, stride=turn_pitch), :].astype(BF16)
                    stage_b[g % 2, c, to, at] = turn[j, pl.ds(GROUP + c, BLOCK, stride=turn_pitch), :].astype(BF16)
            return 0

        per = part_rows // BLOCK
        lax.fori_loop(p * per, (p + 1) * per, block, 0)

    def stage_out(g):
        to = pl.ds(g * GROUP, GROUP)
        return [
            pltpu.make_async_copy(stage_a.at[g % 2], a_own.at[to], sem_st.at[0, g % 2]),
            pltpu.make_async_copy(stage_b.at[g % 2], b_own.at[to], sem_st.at[1, g % 2]),
        ]

    for p in range(parts):
        first_load(p).wait()
        front_part(0, p, first=True)
    for c in stage_out(0):
        c.start()
    pl.semaphore_wait(barrier, 5)

    dirs = [pick(1, 3, 0, 2), pick(0, 1, 1, 0), pick(2, 0, 3, 1), pick(3, 2, 2, 3)]
    hops = [pick(2, 1, 1, 1), pick(2, 1, 1, 1), pick(3, 2, 2, 2), pick(3, 4, 2, 4)]
    src_relay = [3, 2, pick(0, 0, 1, 1), pick(1, 2, 0, 3)]
    tgt = [pick(4, 3, 0, 2), pick(4, 1, 1, 0), pick(2, 0, 5, 1), pick(3, 4, 5, 5)]

    def dev_of(d):
        dx = (d == 0).astype(jnp.int32) + 3 * (d == 1).astype(jnp.int32)
        dy = (d == 2).astype(jnp.int32) + 3 * (d == 3).astype(jnp.int32)
        return (dp, (y + dy) % nc, ((x + dx) % nc) * cores + core)

    perm_devs = [dev_of(d) for d in dirs]

    def tgt_at(k, t):
        to_e = tgt[k] // 4
        return (1 - to_e) * (relay0 + tgt[k] * half + t * h) + to_e * ((2 * t + tgt[k] - 4) * h)

    def remote(src, dst, send, recv, dev):
        return pltpu.make_async_remote_copy(src_ref=src, dst_ref=dst, send_sem=send, recv_sem=recv,
                                            device_id=dev, device_id_type=MESH)

    def perm_copy(k, t, src):
        return remote(src, b_land.at[pl.ds(tgt_at(k, t), h)], sem_sp.at[k, t], sem_rp.at[tgt[k], t], perm_devs[k])

    def got_perm(which, t):
        pltpu.make_async_copy(b_land.at[pl.ds(0, h)], b_land.at[pl.ds(0, h)], sem_rp.at[which, t]).wait()

    def land(buf, slot, t, f=0, count=ch):
        return buf.at[pl.ds(slot * hid + t * ch + f * h, count)]

    def got(buf, sem, count):
        pltpu.make_async_copy(buf.at[pl.ds(0, count)], buf.at[pl.ds(0, count)], sem).wait()

    def own(buf, t, count=ch, f=0):
        return buf.at[pl.ds(t * ch + f * h, count)]

    def a_own_sends(t):
        return [
            remote(own(a_own, t), land(a_land, 0, t), sem_sa.at[0, t], sem_ra.at[0, t], yp),
            remote(own(a_own, t), land(a_land, 1, t), sem_sa.at[1, t], sem_ra.at[1, t], ym),
        ]

    def e_own_sends(t, src):
        return [
            remote(src, land(b_land, 1, t), sem_se.at[0, t], sem_re.at[0, t], xp),
            remote(src, land(b_land, 2, t), sem_se.at[1, t], sem_re.at[1, t], xm),
            remote(src, land(b_land, 4, t), sem_sd.at[0, t], sem_rd.at[0, t], mate),
        ]

    def local_load(t, slot, j):
        put_a = lambda rel: a_buf.at[slot, :, :, pl.ds(rel * cols, cols)]
        out = [
            (own(a_own, t), put_a(0)),
            (land(a_land, 0, t), put_a(3)),
            (land(a_land, 1, t), put_a(1)),
            (land(a_land, 2, t), put_a(2)),
        ]
        for k, delta in enumerate((0, 3, 1, 2)):
            rel = (cls + nc - delta) % nc
            where = pl.ds(pl.multiple_of(rel * cols, 128), cols)
            if k > 0:
                out.append((land(b_land, k, t), b_buf.at[slot, :, core, :, where]))
            out.append((land(b_land, 4 + k, t), b_buf.at[slot, :, 1 - core, :, where]))
        return pltpu.make_async_copy(out[j][0], out[j][1], sem_l.at[slot, j])

    def own_e_load(t, slot, src):
        where = pl.ds(pl.multiple_of(cls * cols, 128), cols)
        return pltpu.make_async_copy(src, b_buf.at[slot, :, core, :, where], sem_l.at[slot, 11])

    def at_lag(q, lag, fn):
        t = q - lag

        @pl.when(jnp.logical_and(t >= 0, t < n))
        def _():
            fn(t)

    gate_rows = rows // (n - 2 * parts)

    def gate_row(first, j, _):
        i = first + j
        s_buf[i] = jax.nn.sigmoid(jnp.dot(w_gate[...], z_buf[i], preferred_element_type=F32))
        return 0

    def drain(t):
        for k in range(4):
            pltpu.make_async_copy(own(b_own, t, h), own(b_own, t, h), sem_sp.at[k, t]).wait()
            pltpu.make_async_copy(own(b_own, t), own(b_own, t), sem_sd.at[k, t]).wait()
        for k in range(4):
            cnt = ch if k < 2 else h
            pltpu.make_async_copy(own(b_own, t, cnt), own(b_own, t, cnt), sem_sa.at[k, t]).wait()
            pltpu.make_async_copy(own(b_own, t, cnt), own(b_own, t, cnt), sem_se.at[k, t]).wait()

    def perm_step(v):
        @pl.when(jnp.logical_and(v < n, v % parts == 0))
        def _():
            for c in stage_out(v // parts):
                c.wait()

        for k in range(4):
            def send(t, k=k):
                if k < 2:
                    @pl.when(is0)
                    def _():
                        got_perm(src_relay[k], t)
                        perm_copy(k, t, b_land.at[pl.ds(relay0 + src_relay[k] * half + t * h, h)]).start()

                    @pl.when(jnp.logical_not(is0))
                    def _():
                        perm_copy(k, t, own(b_own, t, h, k)).start()
                else:
                    got_perm(src_relay[k], t)
                    perm_copy(k, t, b_land.at[pl.ds(relay0 + src_relay[k] * half + t * h, h)]).start()

            at_lag(v, hops[k] - 1, send)

    def front_step(v):
        @pl.when(v < n - parts)
        def _():
            front_part(v // parts + 1, v % parts)

            @pl.when(v % parts == parts - 1)
            def _():
                for c in stage_out(v // parts + 1):
                    c.start()

    def step(q, _):
        early = q < LEAD
        v0 = jnp.where(early, 2 * q, q + LEAD)
        perm_step(v0)

        @pl.when(early)
        def _():
            front_step(2 * q)
            perm_step(2 * q + 1)

        def e_own(t):
            @pl.when(is0)
            def _():
                for c in e_own_sends(t, own(b_own, t)):
                    c.start()

            @pl.when(jnp.logical_not(is0))
            def _():
                got_perm(4, t)
                got_perm(5, t)
                for c in e_own_sends(t, land(b_land, 0, t)):
                    c.start()

        at_lag(q, pick(0, 1, 2, 1), e_own)

        def a_first(t):
            for c in a_own_sends(t):
                c.start()

        at_lag(q, 1, a_first)

        def e_fwd(t):
            got(b_land, sem_re.at[0, t], ch)
            remote(land(b_land, 1, t, 0, h), land(b_land, 3, t, 0, h), sem_se.at[2, t], sem_re.at[2, t], xp).start()
            remote(land(b_land, 1, t), land(b_land, 5, t), sem_sd.at[1, t], sem_rd.at[1, t], mate).start()
            got(b_land, sem_re.at[1, t], ch)
            remote(land(b_land, 2, t, 1, h), land(b_land, 3, t, 1, h), sem_se.at[3, t], sem_re.at[3, t], xm).start()
            remote(land(b_land, 2, t), land(b_land, 6, t), sem_sd.at[2, t], sem_rd.at[2, t], mate).start()

        at_lag(q, 4, e_fwd)

        def a_fwd(t):
            got(a_land, sem_ra.at[0, t], ch)
            remote(land(a_land, 0, t, 0, h), land(a_land, 2, t, 0, h), sem_sa.at[2, t], sem_ra.at[2, t], yp).start()
            got(a_land, sem_ra.at[1, t], ch)
            remote(land(a_land, 1, t, 1, h), land(a_land, 2, t, 1, h), sem_sa.at[3, t], sem_ra.at[3, t], ym).start()

        at_lag(q, 4, a_fwd)

        def last_d2d(t):
            got(b_land, sem_re.at[2, t], h)
            got(b_land, sem_re.at[3, t], h)
            remote(land(b_land, 3, t), land(b_land, 7, t), sem_sd.at[3, t], sem_rd.at[3, t], mate).start()

        at_lag(q, 6, last_d2d)

        late = (3, 9, 10)

        def load_late(t):
            got(a_land, sem_ra.at[2, t], h)
            got(a_land, sem_ra.at[3, t], h)
            got(b_land, sem_rd.at[3, t], ch)
            for j in late:
                local_load(t, t % 2, j).start()

        def load_early(t):
            for k in range(3):
                got(b_land, sem_rd.at[k, t], ch)
            for j in range(11):
                if j not in late:
                    local_load(t, t % 2, j).start()

            @pl.when(is0)
            def _():
                own_e_load(t, t % 2, own(b_own, t)).start()

            @pl.when(jnp.logical_not(is0))
            def _():
                own_e_load(t, t % 2, land(b_land, 0, t)).start()

        at_lag(q, 7, load_late)

        def multiply(t):
            slot = t % 2
            for j in range(11):
                local_load(t, slot, j).wait()
            own_e_load(t, slot, land(b_land, 0, t)).wait()
            pitch = o_buf.shape[1] // hid
            for c in range(ch):
                rhs = b_buf[slot, c].reshape(cores * rows, nc * cols)
                prod = lax.dot_general(a_buf[slot, c], rhs, (((1,), (1,)), ((), ())), preferred_element_type=F32)
                at = pl.ds(pl.multiple_of((t * ch + c) * pitch, 8), rows)
                for j in range(o_buf.shape[0]):
                    o_buf[j, at, :] = prod[:, j * 128:(j + 1) * 128]

        at_lag(q, 8, multiply)
        at_lag(q, 6, load_early)
        at_lag(q, 8, drain)

        front_step(jnp.where(early, 2 * q + 1, q + LEAD))

        @pl.when(q < n - 2 * parts)
        def _():
            lax.fori_loop(0, gate_rows, functools.partial(gate_row, q * gate_rows), 0, unroll=4)

        @pl.when(q == n - parts)
        def _():
            pltpu.make_async_copy(z_hbm, z_buf, sem_z.at[0]).start()

        return 0

    lax.fori_loop(0, n + 8, step, 0)

    pltpu.make_async_copy(z_hbm, z_buf, sem_z.at[0]).wait()
    pitch = o_buf.shape[1] // hid

    def back_row(i, _):
        o = jnp.concatenate([o_buf[j, pl.ds(i, hid, stride=pitch), :] for j in range(o_buf.shape[0])], axis=1)
        on = normalize(o, g_out[:, :1])
        update = jnp.dot(w_out[...], on, preferred_element_type=F32)
        z_buf[i] = (z_buf[i].astype(F32) + s_buf[i] * update).astype(BF16)
        return 0

    per = rows // 8
    for blk in range(8):
        lax.fori_loop(blk * per, (blk + 1) * per, back_row, 0, unroll=BACK_UNROLL)
        pltpu.make_async_copy(z_buf.at[pl.ds(blk * per, per)], out_hbm.at[pl.ds(blk * per, per)], sem_z.at[1 + blk]).start()

    for blk in range(8):
        pltpu.make_async_copy(z_buf.at[pl.ds(blk * per, per)], out_hbm.at[pl.ds(blk * per, per)], sem_z.at[1 + blk]).wait()


def main_call(nc, z_t, mask, small):
    rows, chan, cols = z_t.shape
    hid = chan
    ch = 2 * PER_HALF
    n = hid // ch
    any_spec = pl.BlockSpec(memory_space=pl.ANY)
    vm = pl.BlockSpec(memory_space=pltpu.VMEM)
    dma = lambda *s: pltpu.SemaphoreType.DMA(s)
    return pl.pallas_call(
        functools.partial(main_kernel, nc),
        in_specs=[any_spec] + [vm] * (1 + len(small)),
        out_specs=[any_spec] * 5,
        out_shape=[
            jax.ShapeDtypeStruct(z_t.shape, BF16),
            jax.ShapeDtypeStruct((hid, rows, cols), BF16),
            jax.ShapeDtypeStruct((hid, rows, cols), BF16),
            jax.ShapeDtypeStruct((3 * hid, rows, cols), BF16),
            jax.ShapeDtypeStruct((10 * hid, rows, cols), BF16),
        ],
        scratch_shapes=[
            pltpu.VMEM((2, ch, rows, nc * cols), BF16),
            pltpu.VMEM((2, ch, 2, rows, nc * cols), BF16),
            pltpu.VMEM((cols // 128, hid * (rows + 8), 128), F32),
            pltpu.VMEM(z_t.shape, BF16),
            pltpu.VMEM(z_t.shape, F32),
            pltpu.VMEM((2, GROUP, rows, cols), BF16),
            pltpu.VMEM((2, GROUP, rows, cols), BF16),
            pltpu.VMEM((cols // 128, BLOCK * (2 * GROUP + 8), 128), F32),
            pltpu.VMEM((hid // GROUP, 4 * GROUP, chan), F32),
            pltpu.VMEM((chan, chan), BF16),
            pltpu.VMEM((chan, hid), BF16),
            pltpu.VMEM((chan, chan), F32),
            pltpu.VMEM((hid, hid), F32),
            dma(4, n), dma(6, n), dma(4, n), dma(4, n), dma(4, n), dma(4, n), dma(4, n), dma(4, n),
            dma(2, 12), dma(9), dma(GROUP // ch), dma(2, 2),
        ],
        compiler_params=pltpu.CompilerParams(
            vmem_limit_bytes=VMEM_LIMIT, collective_id=0, has_side_effects=True),
        name="exchange",
    )(z_t, mask, *small)[0]


def copy_kernel(src, dst, buf, sem_a, sem_b):
    parts = sem_a.shape[0]
    per = src.shape[0] // parts

    def take(p):
        at = pl.ds(p * per, per)
        return pltpu.make_async_copy(src.at[at], buf.at[at], sem_a.at[p])

    def put(p):
        at = pl.ds(p * per, per)
        return pltpu.make_async_copy(buf.at[at], dst.at[at], sem_b.at[p])

    for p in range(parts):
        take(p).start()
    for p in range(parts):
        take(p).wait()
        put(p).start()
    for p in range(parts):
        put(p).wait()


def copy_out(v):
    parts = 16
    return pl.pallas_call(
        copy_kernel,
        in_specs=[pl.BlockSpec(memory_space=pl.ANY)],
        out_specs=pl.BlockSpec(memory_space=pl.ANY),
        out_shape=jax.ShapeDtypeStruct(v.shape, v.dtype),
        scratch_shapes=[pltpu.VMEM(v.shape, v.dtype), pltpu.SemaphoreType.DMA((parts,)), pltpu.SemaphoreType.DMA((parts,))],
        compiler_params=pltpu.CompilerParams(vmem_limit_bytes=VMEM_LIMIT),
        name="copy_out",
    )(v)


def solution(mesh):
    nc = mesh.shape['col']
    tile_spec = P(('dp', 'row'), 'col', None)
    mask_spec = P(('dp', 'row'), 'col')

    def tile_program(pair_tile, mask_tile, norm_in, proj_left, gate_left, proj_right, gate_right, proj_gate, norm_out, proj_out):
        z_t = jnp.transpose(pair_tile, (0, 2, 1))
        small = (norm_in[None, :], proj_left, gate_left, proj_right, gate_right, proj_gate, norm_out[None, :], proj_out)
        return jnp.transpose(copy_out(main_call(nc, z_t, mask_tile, small)), (0, 2, 1))

    return jax.shard_map(tile_program, mesh=mesh, in_specs=(tile_spec, mask_spec) + (P(),) * 8, out_specs=tile_spec, check_vma=False)
```
